64 devices in a mesh: rep: 8 (over x, y, core), dp: 8 (over z).
Axes of the slice: x: 2, y: 2, z: 8, core: 2. Of those that a mesh axis runs over, the one named last changes fastest.
The devices are a block of a 4x4x8 slice.
Arguments:
- x: bfloat16 [64, 2048, 512], P(('rep', 'dp')), parts along dimension 0
- dy: bfloat16 [64, 2048, 512], P(('rep', 'dp')), parts along dimension 0
- wq: bfloat16 [2, 512, 512], replicated
- wk: bfloat16 [2, 512, 512], replicated
- wv: bfloat16 [2, 512, 512], replicated
- wo: bfloat16 [2, 512, 512], replicated
- w_gate: bfloat16 [2, 512, 2048], replicated
- w_up: bfloat16 [2, 512, 2048], replicated
- w_down: bfloat16 [2, 2048, 512], replicated
- m_wq: float32 [2, 512, 512], P(None, 'dp')
- m_wk: float32 [2, 512, 512], P(None, 'dp')
- m_wv: float32 [2, 512, 512], P(None, 'dp')
- m_wo: float32 [2, 512, 512], P(None, 'dp')
- m_w_gate: float32 [2, 512, 2048], P(None, 'dp')
- m_w_up: float32 [2, 512, 2048], P(None, 'dp')
- m_w_down: float32 [2, 2048, 512], P(None, 'dp')
- v_wq: float32 [2, 512, 512], P(None, 'dp')
- v_wk: float32 [2, 512, 512], P(None, 'dp')
- v_wv: float32 [2, 512, 512], P(None, 'dp')
- v_wo: float32 [2, 512, 512], P(None, 'dp')
- v_w_gate: float32 [2, 512, 2048], P(None, 'dp')
- v_w_up: float32 [2, 512, 2048], P(None, 'dp')
- v_w_down: float32 [2, 2048, 512], P(None, 'dp')
Outputs:
- output 1: bfloat16 [16, 512, 512], P('rep'), parts along dimension 0
- output 2: bfloat16 [16, 512, 512], P('rep'), parts along dimension 0
- output 3: bfloat16 [16, 512, 512], P('rep'), parts along dimension 0
- output 4: bfloat16 [16, 512, 512], P('rep'), parts along dimension 0
- output 5: bfloat16 [16, 512, 2048], P('rep'), parts along dimension 0
- output 6: bfloat16 [16, 512, 2048], P('rep'), parts along dimension 0
- output 7: bfloat16 [16, 2048, 512], P('rep'), parts along dimension 0
- output 8: float32 [16, 512, 512], P('rep', 'dp'), parts along dimension 0
- output 9: float32 [16, 512, 512], P('rep', 'dp'), parts along dimension 0
- output 10: float32 [16, 512, 512], P('rep', 'dp'), parts along dimension 0
- output 11: float32 [16, 512, 512], P('rep', 'dp'), parts along dimension 0
- output 12: float32 [16, 512, 2048], P('rep', 'dp'), parts along dimension 0
- output 13: float32 [16, 512, 2048], P('rep', 'dp'), parts along dimension 0
- output 14: float32 [16, 2048, 512], P('rep', 'dp'), parts along dimension 0
- output 15: float32 [16, 512, 512], P('rep', 'dp'), parts along dimension 0
- output 16: float32 [16, 512, 512], P('rep', 'dp'), parts along dimension 0
- output 17: float32 [16, 512, 512], P('rep', 'dp'), parts along dimension 0
- output 18: float32 [16, 512, 512], P('rep', 'dp'), parts along dimension 0
- output 19: float32 [16, 512, 2048], P('rep', 'dp'), parts along dimension 0
- output 20: float32 [16, 512, 2048], P('rep', 'dp'), parts along dimension 0
- output 21: float32 [16, 2048, 512], P('rep', 'dp'), parts along dimension 0
There are 8 independent parts. The reference program is written for one: setup_inputs(seed, part) draws one part's arguments, and reference() takes and returns one part's arrays. A program takes and returns all parts, laid end to end along the dimension named above; an argument that names none is the same for every part.
All inputs are finite; a program needn't handle non-finite values.
Results may differ from the reference program's by a relative error of at most 0.024.
Values are sent between devices in bfloat16 or wider.
A program may use at most 768 MiB of HBM per device.

```python
import jax
import jax.numpy as jnp
from jax import lax

SEQUENCES = 8
TOKENS = 2048
D = 512
HEADS = 4
KV_HEADS = 4
HEAD = 128
FF = 2048
LAYERS = 2
THETA = 10000
NAMES = ("wq", "wk", "wv", "wo", "w_gate", "w_up", "w_down")
SHAPES = {
    "wq": (LAYERS, D, HEADS * HEAD),
    "wk": (LAYERS, D, KV_HEADS * HEAD),
    "wv": (LAYERS, D, KV_HEADS * HEAD),
    "wo": (LAYERS, HEADS * HEAD, D),
    "w_gate": (LAYERS, D, FF),
    "w_up": (LAYERS, D, FF),
    "w_down": (LAYERS, FF, D),
}


def bump(key, n, height):
    away = (jnp.arange(n, dtype=jnp.int32) - jax.random.randint(key, (), 0, n, jnp.int32)) % n
    return jnp.where(away < n // 8, height, 1.0)


def together(key, own, strength):
    shared = jax.random.normal(key, own.shape[1:], jnp.float32)
    return (own + strength * shared) * lax.rsqrt(1 + strength * strength)


def setup_inputs(seed: int = 0, part: int = 0) -> dict:
    kx, kdy, ka, kb, kz, kf, kh, kl, *keys = jax.random.split(jax.random.key(seed), 8 + 3 * len(NAMES))
    kx, kdy, ka, kb = (jax.random.fold_in(k, part) for k in (kx, kdy, ka, kb))
    kw, km, kv = (keys[i::3] for i in range(3))
    shape = (SEQUENCES, TOKENS, D)
    much_x, much_dy = jax.random.uniform(kz, (2,), jnp.float32, 0.0, 1.0)
    loud = 2.0 ** jax.random.uniform(jax.random.fold_in(kz, 1), (), jnp.float32, -1.0, 2.0)
    layers = 2.0 ** jax.random.uniform(kl, (LAYERS, 1, 1), jnp.float32, -1.0, 1.0)
    times = {"wq": 1.0, "wk": 1.0, "wv": 2.0, "wo": layers, "w_gate": 1.0, "w_up": bump(kh, FF, 4.0), "w_down": layers}
    x = together(ka, jax.random.normal(kx, shape, jnp.float32), much_x) * bump(kf, D, 4.0)
    dy = together(kb, jax.random.normal(kdy, shape, jnp.float32), much_dy)
    drawn = {"x": x.astype(jnp.bfloat16), "dy": (loud * dy * (SEQUENCES * TOKENS) ** -0.5).astype(jnp.bfloat16)}
    for key, name in zip(kw, NAMES, strict=True):
        drawn[name] = (jax.random.normal(key, SHAPES[name], jnp.float32) * SHAPES[name][1] ** -0.5 * times[name]).astype(jnp.bfloat16)
    for key, name in zip(km, NAMES, strict=True):
        drawn[f"m_{name}"] = 0.1 * jax.random.normal(key, SHAPES[name], jnp.float32)
    for key, name in zip(kv, NAMES, strict=True):
        drawn[f"v_{name}"] = loud * loud * jax.random.uniform(key, SHAPES[name], jnp.float32, 0.2, 0.6)
    return drawn


def matmul(a, w):
    return jnp.dot(a, w, preferred_element_type=jnp.float32).astype(jnp.bfloat16)


def normed(h):
    wide = h.astype(jnp.float32)
    scale = lax.rsqrt(jnp.mean(wide**2, -1, keepdims=True) + 1e-6)
    return (wide * scale).astype(jnp.bfloat16)


def turned(t, theta):
    half = t.shape[-1] // 2
    angle = jnp.arange(t.shape[0], dtype=jnp.float32)[:, None] * theta ** (-jnp.arange(half, dtype=jnp.float32) / half)
    cos, sin = jnp.cos(angle)[:, None], jnp.sin(angle)[:, None]
    a, b = t[..., :half].astype(jnp.float32), t[..., half:].astype(jnp.float32)
    return jnp.concatenate([a * cos - b * sin, b * cos + a * sin], -1).astype(jnp.bfloat16)


def seen_by(q, k, v):
    tokens, kv = q.shape[0], k.shape[1]
    q = q.reshape(tokens, kv, -1, q.shape[-1])
    scores = jnp.einsum("tgsd,ugd->gstu", q.astype(jnp.float32), k.astype(jnp.float32)) * q.shape[-1] ** -0.5
    place = jnp.arange(tokens)
    weights = jax.nn.softmax(jnp.where(place[:, None] >= place, scores, -jnp.inf), -1).astype(jnp.bfloat16)
    return jnp.einsum("gstu,ugd->tgsd", weights.astype(jnp.float32), v.astype(jnp.float32)).astype(jnp.bfloat16).reshape(tokens, -1)


def layer(h, w):
    a = normed(h)
    q, k = (turned(matmul(a, w[name]).reshape(h.shape[0], -1, HEAD), THETA) for name in ("wq", "wk"))
    h = h + matmul(seen_by(q, k, matmul(a, w["wv"]).reshape(h.shape[0], -1, HEAD)), w["wo"])
    b = normed(h)
    gate = jnp.dot(b, w["w_gate"], preferred_element_type=jnp.float32)
    up = jnp.dot(b, w["w_up"], preferred_element_type=jnp.float32)
    return h + matmul((jax.nn.silu(gate) * up).astype(jnp.bfloat16), w["w_down"])


def adamw(w, m, v, g):
    m = 0.9 * m + 0.1 * g
    v = 0.95 * v + 0.05 * g * g
    step = m * lax.rsqrt(v + 1e-8) + 0.1 * w
    return (w - 0.02 * step).astype(jnp.bfloat16), m, v


def stack(weights, h):
    return lax.scan(lambda h, w: (layer(h, w), None), h, weights)[0]


def reference(x, dy, wq, wk, wv, wo, w_gate, w_up, w_down, m_wq, m_wk, m_wv, m_wo, m_w_gate, m_w_up, m_w_down, v_wq, v_wk, v_wv, v_wo, v_w_gate, v_w_up, v_w_down):
    weights = dict(zip(NAMES, (wq, wk, wv, wo, w_gate, w_up, w_down), strict=True))

    def take(so_far, sequence):
        h, by_y = sequence
        _, back = jax.vjp(stack, weights, h)
        by_weights, by_h = back(by_y)
        return jax.tree.map(lambda total, term: total + term.astype(jnp.float32), so_far, by_weights), by_h

    none_yet = {name: jnp.zeros(w.shape, jnp.float32) for name, w in weights.items()}
    by_weights, by_x = lax.scan(take, none_yet, (x, dy))
    gradients = [by_weights[name].astype(jnp.bfloat16).astype(jnp.float32) for name in NAMES]
    first = (m_wq, m_wk, m_wv, m_wo, m_w_gate, m_w_up, m_w_down)
    second = (v_wq, v_wk, v_wv, v_wo, v_w_gate, v_w_up, v_w_down)
    new = [adamw(weights[name].astype(jnp.float32), m, v, g) for name, m, v, g in zip(NAMES, first, second, gradients, strict=True)]
    return tuple(one[which] for which in range(3) for one in new)
```

```python
import functools

import jax
import jax.numpy as jnp
import numpy as np
from jax import lax
from jax.experimental import pallas as pl
from jax.experimental.pallas import tpu as pltpu
from jax.sharding import PartitionSpec as P

F32, BF16 = jnp.float32, jnp.bfloat16


HEAD = 128
THETA = 10000
LOG2E = 1.4426950408889634
NEG = -1e30
HIDDEN = 2 * NEG
TB = 512


def dot(a, b, ca=1, cb=0):
    return lax.dot_general(a, b, (((ca,), (cb,)), ((), ())), preferred_element_type=F32)


def rotary_tables(tokens):
    half = HEAD // 2
    rate = float(THETA) ** (-np.arange(half) / half)
    rate = np.concatenate([rate, rate])
    turn = np.concatenate([-np.ones(half), np.ones(half)])
    big = np.arange(tokens // 64)[:, None] * 64.0 * rate
    small = np.arange(64)[:, None] * rate
    return [jnp.asarray(t, F32) for t in (np.cos(big), np.sin(big), np.cos(small), np.sin(small))], jnp.asarray(turn[None], F32)


def fill_rotary(tabs, at, cos_s, sin_s):
    cb_ref, sb_ref, cs_ref, ss_ref, turn_ref = tabs
    cs, ss, turn = cs_ref[...], ss_ref[...], turn_ref[...]
    for n in range(TB // 64):
        cb, sb = cb_ref[pl.ds(at * (TB // 64) + n, 1), :], sb_ref[pl.ds(at * (TB // 64) + n, 1), :]
        cos_s[n * 64 : n * 64 + 64, :] = cb * cs - sb * ss
        sin_s[n * 64 : n * 64 + 64, :] = (sb * cs + cb * ss) * turn


def rotated(t, cos, sin):
    return t * cos + pltpu.roll(t, HEAD // 2, 1) * sin


def normed(h):
    wide = h.astype(F32)
    scale = lax.rsqrt(jnp.mean(wide * wide, -1, keepdims=True) + 1e-6)
    return (wide * scale).astype(BF16)


def attend_block(nb, q_s, k_ref, v_ref, o_put, lse_put, top_s, mix_s):
    heads = q_s.shape[1] // HEAD
    e = HEAD**-0.5 * LOG2E
    ones = jnp.ones((8, TB), BF16)

    def block(j, masked, first):
        here = pl.ds(pl.multiple_of(j * TB, TB), TB)
        scores = [dot(k_ref[here, h * HEAD : h * HEAD + HEAD], q_s[:, h * HEAD : h * HEAD + HEAD], 1, 1) for h in range(heads)]
        if masked:
            ok = lax.broadcasted_iota(jnp.int32, (TB, TB), 1) >= lax.broadcasted_iota(jnp.int32, (TB, TB), 0)
        weights, keeps = [], []
        for h, s in enumerate(scores):
            if masked:
                s = jnp.where(ok, s, HIDDEN)
            top = s.max(axis=0, keepdims=True)
            if not first:
                old = top_s[h : h + 1, :]
                top = jnp.maximum(old, top)
                keeps.append(jnp.exp2((old - top) * e))
            top_s[h : h + 1, :] = top
            weights.append(jnp.exp2((s - top) * e).astype(BF16))
        for h, p in enumerate(weights):
            values = jnp.concatenate([v_ref[here, h * HEAD : h * HEAD + HEAD].T, ones], axis=0)
            got = dot(values, p)
            mix_s[h] = got if first else mix_s[h] * keeps[h] + got

    block(nb, True, True)
    lax.fori_loop(0, nb, lambda j, _: block(j, False, False), None)
    for h in range(heads):
        total = mix_s[h, HEAD : HEAD + 1, :]
        o_put(h, (mix_s[h, :HEAD, :] * (1 / total)).T.astype(BF16))
        lse_put(h, top_s[h : h + 1, :] * (HEAD**-0.5) + jnp.log(total))


def forward_kernel(x_ref, wq_ref, wk_ref, wv_ref, wo_ref, wg_ref, wu_ref, wd_ref, *rest, ff):
    tabs, rest = rest[:5], rest[5:]
    a_ref, q_ref, k_ref, v_ref, o_ref, lse_ref, hm_ref, b_ref, h1_ref = rest[:9]
    ks, vs, cos_s, sin_s, top_s, mix_s = rest[9:]
    i = pl.program_id(0)
    heads = q_ref.shape[-1] // HEAD
    here = pl.ds(pl.multiple_of(i * TB, TB), TB)
    fill_rotary(tabs, i, cos_s, sin_s)

    def attention_part(layer, h):
        a = normed(h)
        a_ref[layer] = a
        for w_ref, out, kept in ((wq_ref, q_ref, None), (wk_ref, k_ref, ks), (wv_ref, v_ref, vs)):
            t = dot(a, w_ref[layer]).astype(BF16)
            if out is not v_ref:
                cos, sin = cos_s[...], sin_s[...]
                wide = t.astype(F32)
                t = jnp.concatenate([rotated(wide[:, n * HEAD : n * HEAD + HEAD], cos, sin) for n in range(heads)], axis=1).astype(BF16)
            out[layer] = t
            if kept is not None:
                kept[layer, here, :] = t

        def o_put(n, o):
            o_ref[layer, :, n * HEAD : n * HEAD + HEAD] = o

        def lse_put(n, lse):
            lse_ref[layer, n : n + 1, :] = lse

        attend_block(i, q_ref.at[layer], ks.at[layer], vs.at[layer], o_put, lse_put, top_s, mix_s)
        hm = h + dot(o_ref[layer], wo_ref[layer]).astype(BF16)
        hm_ref[layer] = hm
        b = normed(hm)
        b_ref[layer] = b
        return hm, b

    hm, b = attention_part(0, x_ref[...])
    total = None
    step = 512
    for n in range(0, ff, step):
        gate, up = dot(b, wg_ref[0, :, n : n + step]), dot(b, wu_ref[0, :, n : n + step])
        part = dot((gate * jax.nn.sigmoid(gate) * up).astype(BF16), wd_ref[0, n : n + step, :])
        total = part if total is None else total + part
    h1 = hm + total.astype(BF16)
    h1_ref[...] = h1
    attention_part(1, h1)


def forward(x, wq, wk, wv, wo, wg, wu, wd):
    tokens, d = x.shape
    ff = wg.shape[2]
    hd = wq.shape[2]
    heads = hd // HEAD
    tabs, turn = rotary_tables(tokens)
    whole = lambda a: pl.BlockSpec(a.shape, lambda i: (0,) * a.ndim, pipeline_mode=pl.Buffered(1))
    one = lambda a: pl.BlockSpec((1, *a.shape[1:]), lambda i: (0,) * a.ndim, pipeline_mode=pl.Buffered(1))
    both = pl.BlockSpec((2, TB, d), lambda i: (0, i, 0))
    args = [x, wq, wk, wv, wo, wg, wu, wd, *tabs, turn]
    specs = [pl.BlockSpec((TB, d), lambda i: (i, 0)), *(whole(w) for w in (wq, wk, wv, wo)), *(one(w) for w in (wg, wu, wd)), *(whole(t) for t in (*tabs, turn))]
    big = jax.ShapeDtypeStruct((2, tokens, d), BF16)
    outs = [big] * 5 + [jax.ShapeDtypeStruct((2, heads, tokens), F32), big, big, jax.ShapeDtypeStruct((tokens, d), BF16)]
    ospecs = [both] * 5 + [pl.BlockSpec((2, heads, TB), lambda i: (0, 0, i)), both, both, pl.BlockSpec((TB, d), lambda i: (i, 0))]
    return pl.pallas_call(
        functools.partial(forward_kernel, ff=ff),
        grid=(tokens // TB,),
        in_specs=specs, out_specs=ospecs, out_shape=outs,
        scratch_shapes=[pltpu.VMEM((2, tokens, hd), BF16), pltpu.VMEM((2, tokens, hd), BF16), pltpu.VMEM((TB, HEAD), F32), pltpu.VMEM((TB, HEAD), F32),
                        pltpu.VMEM((heads, TB), F32), pltpu.VMEM((heads, HEAD + 8, TB), F32)],
        compiler_params=pltpu.CompilerParams(dimension_semantics=("arbitrary",), vmem_limit_bytes=60 * 2**20),
        name="forward",
    )(*args)

N = 8
ROWS, COLS = 64, 512
SLOTS = 8
MESH = pl.DeviceIdType.MESH


class Ring:
    def __init__(self, axis, count, terms, rs, ag, rs_send, rs_recv, ag_send, ag_recv, term_at, update, store, stored):
        self.axis, self.count = axis, count
        self.terms, self.rs, self.ag = terms, rs, ag
        self.sems = rs_send, rs_recv, ag_send, ag_recv
        self.term_at, self.update, self.store, self.stored = term_at, update, store, stored
        self.me = lax.axis_index(axis)

    def at(self, offset):
        return lax.rem(self.me + offset + 2 * N, N)

    def barrier(self):
        sem = pltpu.get_barrier_semaphore()
        for d in (1, -1):
            pl.semaphore_signal(sem, inc=1, device_id={self.axis: self.at(d)}, device_id_type=MESH)
        pl.semaphore_wait(sem, 2)

    def sign(self, c):
        return 1 - 2 * lax.rem(c, 2)

    def sum_copy(self, c, s, far):
        d = self.sign(c) * (1 if far else -1)
        hops = 4 if far else 3
        at, slot = lax.rem(c, SLOTS), (0 if far else 4) + s - 1
        block = self.at(d * (hops - s + 1))
        src = self.terms.at[self.term_at(c), block] if s == 1 else self.rs.at[at, slot - 1]
        return pltpu.make_async_remote_copy(src_ref=src, dst_ref=self.rs.at[at, slot], send_sem=self.sems[0].at[at, slot], recv_sem=self.sems[1].at[at, slot],
                                            device_id={self.axis: self.at(d)}, device_id_type=MESH)

    def new_copy(self, c, s, far):
        d = self.sign(c) * (1 if far else -1)
        at, slot = lax.rem(c, SLOTS), (0 if far else 4) + s - 1
        src = self.ag.at[at, 7] if s == 1 else self.ag.at[at, slot - 1]
        return pltpu.make_async_remote_copy(src_ref=src, dst_ref=self.ag.at[at, slot], send_sem=self.sems[2].at[at, slot], recv_sem=self.sems[3].at[at, slot],
                                            device_id={self.axis: self.at(d)}, device_id_type=MESH)

    def sum_step(self, c, age):
        for far in (True, False):
            hops = 4 if far else 3
            if age > hops:
                continue
            if age > 0:
                was = self.sum_copy(c, age, far)
                was.wait()
            if 0 < age < hops:
                d = self.sign(c) * (1 if far else -1)
                block, at, slot = self.at(d * (hops - age)), lax.rem(c, SLOTS), (0 if far else 4) + age - 1
                own, got = self.terms.at[self.term_at(c), block], self.rs.at[at, slot]
                got[...] = (got[...].astype(F32) + own[...].astype(F32)).astype(BF16)
            if age < hops:
                self.sum_copy(c, age + 1, far).start()
        if age == 4:
            at = lax.rem(c, SLOTS)
            g = self.terms[self.term_at(c), self.me].astype(F32) + self.rs[at, 3].astype(F32) + self.rs[at, 6].astype(F32)
            self.ag[at, 7] = self.update(c, g.astype(BF16).astype(F32))

    def new_step(self, c, age):
        d0 = self.sign(c)
        at = lax.rem(c, SLOTS)
        for far in (True, False):
            hops, d = (4, d0) if far else (3, -d0)
            if age > hops:
                continue
            if age > 0:
                self.new_copy(c, age, far).wait()
            if age < hops:
                self.new_copy(c, age + 1, far).start()
            if age > 0:
                self.store(c, (0 if far else 4) + age - 1, self.at(-d * age))
        if age == 0:
            self.store(c, 7, self.me)

    def tick(self, t):
        ok = lambda c: (c >= 0) & (c < self.count)
        @pl.when(ok(t - 10))
        def _(): self.stored(t - 10)
        for age in range(5):
            @pl.when(ok(t - age))
            def _(age=age): self.sum_step(t - age, age)
        for age in range(5):
            @pl.when(ok(t - 4 - age))
            def _(age=age): self.new_step(t - 4 - age, age)

FB = 256
PER = 16
KEEP = 4


def norm_back(by_n, h):
    scale = lax.rsqrt(jnp.mean(h * h, -1, keepdims=True) + 1e-6)
    return by_n * scale - h * (scale * scale * scale * jnp.mean(by_n * h, -1, keepdims=True))


def backward_kernel(*refs, axis, tokens, d, ff, layers):
    (dy_h, b_h, hm_h, a_h, q_h, k_h, v_h, o_h, lse_h, h1_h), refs = refs[:10], refs[10:]
    weights_h, m_h, v2_h, tabs, refs = refs[:7], refs[7:14], refs[14:21], refs[21:26], refs[26:]
    new_h, nm_h, nv_h, refs = refs[:7], refs[7:14], refs[14:21], refs[21:]
    (S1, S2, S3, S4, S5, S6, S7, S8, F1, F2, dq_s, lse_s, delta_s, wa_s, wgu_s, wd_s, cos_s, sin_s,
     terms, rs, ag, mw_s, mo_s, w_s, rs_send, rs_recv, ag_send, ag_recv, in_sem, out_sem, mo_sem, act_sem, slab_sem) = refs
    wq_h, wk_h, wv_h, wo_h, wg_h, wu_h, wd_h = weights_h
    heads = d // HEAD
    steps, blocks = ff // FB, tokens // TB
    count = layers * PER
    me = lax.axis_index(axis)

    def kinds(c):
        k = lax.rem(c, PER)
        layer = layers - 1 - lax.div(c, PER)
        return k, layer

    def places(c, owner, arrays, mine):
        k, layer = kinds(c)
        q, kk, v, o, g, u, dn = arrays
        own = 0 if mine else owner
        slab = pl.ds(pl.multiple_of(jnp.minimum(k, steps - 1) * FB, FB), FB)
        rows = pl.ds(pl.multiple_of(own * ROWS, ROWS), ROWS)
        strip = pl.ds(pl.multiple_of(own * (ff // N) + jnp.clip(k - steps, 0, 3) * ROWS, ROWS), ROWS)
        out = [(k < steps, [(g.at[layer, rows, slab], 0, FB), (u.at[layer, rows, slab], FB, FB)]),
               ((k >= steps) & (k < steps + 4), [(dn.at[layer, strip, :], 0, COLS)])]
        for n, ref in enumerate((o, q, kk, v)):
            out.append((k == steps + 4 + n, [(ref.at[layer, rows, :], 0, COLS)]))
        return out

    def fetch(c):
        at = lax.rem(c, KEEP)
        for n, arrays in enumerate((m_h, v2_h)):
            for cond, parts in places(c, me, arrays, True):
                @pl.when(cond)
                def _():
                    for ref, col, cols in parts:
                        pltpu.make_async_copy(ref, mw_s.at[at, n, :, pl.ds(col, cols)], in_sem.at[at, n]).start()
        for cond, parts in places(c, me, weights_h, False):
            @pl.when(cond)
            def _():
                for ref, col, cols in parts:
                    pltpu.make_async_copy(ref, w_s.at[at, :, pl.ds(col, cols)], in_sem.at[at, 2]).start()

    def put_state(c):
        at = lax.rem(c, KEEP)
        for n, arrays in enumerate((nm_h, nv_h)):
            for cond, parts in places(c, me, arrays, True):
                @pl.when(cond)
                def _():
                    for ref, col, cols in parts:
                        pltpu.make_async_copy(mo_s.at[at, n, :, pl.ds(col, cols)], ref, mo_sem.at[at, n]).start()

    def state_done(c):
        at = lax.rem(c, KEEP)
        for n in range(2):
            pltpu.make_async_copy(mo_s.at[at, n], mw_s.at[at, n], mo_sem.at[at, n]).wait()

    def update(c, g):
        at = lax.rem(c, KEEP)
        for n in range(2):
            pltpu.make_async_copy(mo_s.at[at, n], mw_s.at[at, n], in_sem.at[at, n]).wait()
        pltpu.make_async_copy(w_s.at[at], w_s.at[at], in_sem.at[at, 2]).wait()
        m = 0.9 * mw_s[at, 0] + 0.1 * g
        v = 0.95 * mw_s[at, 1] + 0.05 * g * g
        w = w_s[at].astype(F32)
        mo_s[at, 0] = m
        mo_s[at, 1] = v
        put_state(c)
        return (w - 0.02 * (m * lax.rsqrt(v + 1e-8) + 0.1 * w)).astype(BF16)

    def store(c, slot, block):
        at = lax.rem(c, SLOTS)
        for cond, parts in places(c, block, new_h, False):
            @pl.when(cond)
            def _():
                for ref, col, cols in parts:
                    pltpu.make_async_copy(ag.at[at, slot, :, pl.ds(col, cols)], ref, out_sem.at[at]).start()

    def stored(c):
        at = lax.rem(c, SLOTS)
        pltpu.make_async_copy(ag.at[at], ag.at[at], out_sem.at[at]).wait()

    ring = Ring(axis, count, terms, rs, ag, rs_send, rs_recv, ag_send, ag_recv, lambda c: lax.rem(c, PER), update, store, stored)
    within = lambda c: (c >= 0) & (c < count)

    def tick(t):
        @pl.when(within(t - 2))
        def _(): fetch(t - 2)
        @pl.when(within(t - 4 - KEEP + 1))
        def _(): state_done(t - 4 - KEEP + 1)
        ring.tick(t)

    def slab(layer, j, at):
        here = pl.ds(pl.multiple_of(j * FB, FB), FB)
        return [pltpu.make_async_copy(wg_h.at[layer, :, here], wgu_s.at[at, :, 0:FB], slab_sem.at[at, 0]),
                pltpu.make_async_copy(wu_h.at[layer, :, here], wgu_s.at[at, :, FB : 2 * FB], slab_sem.at[at, 1]),
                pltpu.make_async_copy(wd_h.at[layer, here, :], wd_s.at[at], slab_sem.at[at, 2])]

    def load(n, ref, dst):
        return pltpu.make_async_copy(ref, dst, act_sem.at[n])

    def attention_weights(layer):
        return [load(8 + n, w.at[layer], wa_s.at[n]) for n, w in enumerate((wq_h, wk_h, wv_h, wo_h))]

    top = layers - 1
    load(0, b_h.at[top], S1).start()
    load(1, dy_h, S2).start()
    for copy in slab(top, 0, 0):
        copy.start()
    ring.barrier()
    load(1, dy_h, S2).wait()

    def mlp_step(p, layer, j):
        at = lax.rem(j, 2)
        for copy in slab(layer, j, at):
            copy.wait()
        @pl.when(j + 1 < steps)
        def _():
            for copy in slab(layer, j + 1, 1 - at):
                copy.start()

        def part(i, _):
            here = pl.ds(pl.multiple_of(i * TB, TB), TB)
            w = wgu_s[at]
            gu = dot(S1[here, :], w)
            by_act = dot(S2[here, :], wd_s[at], 1, 1).astype(BF16).astype(F32)
            gate, up = gu[:, :FB], gu[:, FB:]
            s = jax.nn.sigmoid(gate)
            gs = gate * s
            S4[here, 0:FB] = (gs * up).astype(BF16)
            by = jnp.concatenate([by_act * up * (s + gs * (1 - s)), by_act * gs], axis=1).astype(BF16)
            S3[here, :] = by
            got = dot(by, w, 1, 1)
            @pl.when(j == 0)
            def _(): F1[here, :] = got
            @pl.when(j > 0)
            def _(): F1[here, :] += got

        lax.fori_loop(0, blocks, part, None)
        by_gu = dot(S1[...], S3[...], 0, 0).astype(BF16)
        by_d = dot(S4[:, 0:FB], S2[...], 0, 0).astype(BF16)
        for r in range(N):
            terms[j, r] = by_gu[r * ROWS : (r + 1) * ROWS, :]
        for r in range(FB // ROWS):
            terms[steps + r, j] = by_d[r * ROWS : (r + 1) * ROWS, :]
        tick(p * PER + j)

    def put_terms(k, by_w):
        for r in range(N):
            terms[k, r] = by_w[r * ROWS : (r + 1) * ROWS, :]

    def turned_back(t, cos, sin):
        parts = [rotated(t[:, n * HEAD : n * HEAD + HEAD], cos, -sin) for n in range(heads)]
        return jnp.concatenate(parts, axis=1).astype(BF16)

    def one_layer(p, _):
        layer = layers - 1 - p
        for copy in attention_weights(layer):
            copy.start()
        load(2, hm_h.at[layer], S8).start()
        load(3, o_h.at[layer], S5).start()
        load(4, a_h.at[layer], S7).start()
        load(5, lse_h.at[layer], lse_s).start()
        load(0, b_h.at[layer], S1).wait()
        lax.fori_loop(0, steps, lambda j, _: mlp_step(p, layer, j), None)
        load(0, q_h.at[layer], S1).start()
        load(6, k_h.at[layer], S3).start()
        load(7, v_h.at[layer], S4).start()
        for copy in attention_weights(layer):
            copy.wait()
        load(2, hm_h.at[layer], S8).wait()
        load(3, o_h.at[layer], S5).wait()
        load(5, lse_h.at[layer], lse_s).wait()

        def into_attention(i, _):
            here = pl.ds(pl.multiple_of(i * TB, TB), TB)
            by_b = F1[here, :].astype(BF16).astype(F32)
            back = norm_back(by_b, S8[here, :].astype(F32)).astype(BF16)
            by_hm = (S2[here, :].astype(F32) + back.astype(F32)).astype(BF16)
            S2[here, :] = by_hm
            by_o = dot(by_hm, wa_s[3], 1, 1).astype(BF16)
            S6[here, :] = by_o
            both = (by_o.astype(F32) * S5[here, :].astype(F32)).T
            for h in range(heads):
                delta_s[h : h + 1, here] = both[h * HEAD : h * HEAD + HEAD, :].sum(axis=0, keepdims=True)

        lax.fori_loop(0, blocks, into_attention, None)
        put_terms(steps + 4, dot(S5[...], S2[...], 0, 0).astype(BF16))
        load(0, q_h.at[layer], S1).wait()
        load(6, k_h.at[layer], S3).wait()
        load(7, v_h.at[layer], S4).wait()

        e = HEAD**-0.5 * LOG2E

        def pair(i, j, masked):
            qs = pl.ds(pl.multiple_of(i * TB, TB), TB)
            ks = pl.ds(pl.multiple_of(j * TB, TB), TB)
            cols = [slice(h * HEAD, h * HEAD + HEAD) for h in range(heads)]
            scores = [dot(S3[ks, c], S1[qs, c], 1, 1) for c in cols]
            dps = [dot(S4[ks, c], S6[qs, c], 1, 1) for c in cols]
            if masked:
                ok = lax.broadcasted_iota(jnp.int32, (TB, TB), 1) >= lax.broadcasted_iota(jnp.int32, (TB, TB), 0)
            for h, c in enumerate(cols):
                prob = jnp.exp2(scores[h] * e - lse_s[h : h + 1, qs] * LOG2E)
                if masked:
                    prob = jnp.where(ok, prob, 0.0)
                ds = (prob * (dps[h] - delta_s[h : h + 1, qs])).astype(BF16)
                by_v = dot(prob.astype(BF16), S6[qs, c])
                by_k = dot(ds, S1[qs, c])
                if masked:
                    F2[ks, c] = by_v
                    F1[ks, c] = by_k
                else:
                    F2[ks, c] += by_v
                    F1[ks, c] += by_k
                dq_s[h] += dot(S3[ks, c].T, ds)

        def flat(n, _):
            i = (n >= 1).astype(jnp.int32) + (n >= 3).astype(jnp.int32) + (n >= 6).astype(jnp.int32)
            j = n - lax.div(i * (i + 1), 2)
            @pl.when(j == 0)
            def _(): dq_s[...] = jnp.zeros_like(dq_s)
            @pl.when(j < i)
            def _(): pair(i, j, False)
            @pl.when(j == i)
            def _():
                pair(i, j, True)
                qs = pl.ds(pl.multiple_of(i * TB, TB), TB)
                fill_rotary(tabs, i, cos_s, sin_s)
                by_q = jnp.concatenate([(dq_s[h] * HEAD**-0.5).T for h in range(heads)], axis=1).astype(BF16).astype(F32)
                S5[qs, :] = turned_back(by_q, cos_s[...], sin_s[...])
            @pl.when(lax.rem(n, 2) == 1)
            def _(): tick(p * PER + steps + lax.div(n, 2))

        lax.fori_loop(0, blocks * (blocks + 1) // 2, flat, None)

        @pl.when(p + 1 < layers)
        def _():
            load(0, b_h.at[layer - 1], S1).start()
            for copy in slab(layer - 1, 0, 0):
                copy.start()
            load(2, h1_h, S8).start()

        def out_of_attention(i, _):
            here = pl.ds(pl.multiple_of(i * TB, TB), TB)
            fill_rotary(tabs, i, cos_s, sin_s)
            S3[here, :] = turned_back((F1[here, :] * HEAD**-0.5).astype(BF16).astype(F32), cos_s[...], sin_s[...])
            S4[here, :] = F2[here, :].astype(BF16)

        lax.fori_loop(0, blocks, out_of_attention, None)
        load(4, a_h.at[layer], S7).wait()
        for n, ref in enumerate((S5, S3, S4)):
            put_terms(steps + 5 + n, dot(S7[...], ref[...], 0, 0).astype(BF16))
            tick(p * PER + steps + 5 + n)

        @pl.when(p + 1 < layers)
        def _():
            load(2, h1_h, S8).wait()

            def into_layer(i, _):
                here = pl.ds(pl.multiple_of(i * TB, TB), TB)
                by_a = sum(dot(ref[here, :], wa_s[n], 1, 1) for n, ref in enumerate((S5, S3, S4))).astype(BF16).astype(F32)
                back = norm_back(by_a, S8[here, :].astype(F32)).astype(BF16)
                S2[here, :] = (S2[here, :].astype(F32) + back.astype(F32)).astype(BF16)

            lax.fori_loop(0, blocks, into_layer, None)

    lax.fori_loop(0, layers, one_layer, None)
    lax.fori_loop(count, count + 11, lambda t, _: tick(t), None)


def backward(axis, dy, kept, h1, weights, m, v):
    layers, tokens, d = kept[0].shape
    ff = weights[4].shape[2]
    tabs, turn = rotary_tables(tokens)
    args = [dy, *kept, h1, *weights, *m, *v, *tabs, turn]
    anywhere = pl.BlockSpec(memory_space=pl.ANY)
    inside = pl.BlockSpec(memory_space=pltpu.VMEM)
    shape = lambda a, t=None: jax.ShapeDtypeStruct(a.shape, t or a.dtype)
    big = lambda t: pltpu.VMEM((tokens, d), t)
    sem = pltpu.SemaphoreType.DMA
    outs = pl.pallas_call(
        functools.partial(backward_kernel, axis=axis, tokens=tokens, d=d, ff=ff, layers=layers),
        in_specs=[anywhere] * (len(args) - 5) + [inside] * 5,
        out_specs=[anywhere] * 21,
        out_shape=[*(shape(w) for w in weights), *(shape(a) for a in m), *(shape(a) for a in v)],
        scratch_shapes=[*(big(BF16) for _ in range(8)), big(F32), big(F32), pltpu.VMEM((d // HEAD, HEAD, TB), F32),
                        pltpu.VMEM((d // HEAD, tokens), F32), pltpu.VMEM((d // HEAD, tokens), F32), pltpu.VMEM((4, d, d), BF16),
                        pltpu.VMEM((2, d, 2 * FB), BF16), pltpu.VMEM((2, FB, d), BF16), pltpu.VMEM((TB, HEAD), F32), pltpu.VMEM((TB, HEAD), F32),
                        pltpu.VMEM((PER, N, ROWS, COLS), BF16), pltpu.VMEM((SLOTS, 7, ROWS, COLS), BF16), pltpu.VMEM((SLOTS, 8, ROWS, COLS), BF16),
                        pltpu.VMEM((KEEP, 2, ROWS, COLS), F32), pltpu.VMEM((KEEP, 2, ROWS, COLS), F32), pltpu.VMEM((KEEP, ROWS, COLS), BF16),
                        sem((SLOTS, 7)), sem((SLOTS, 7)), sem((SLOTS, 7)), sem((SLOTS, 7)), sem((KEEP, 3)), sem((SLOTS,)), sem((KEEP, 2)), sem((12,)), sem((2, 3))],
        compiler_params=pltpu.CompilerParams(collective_id=0, has_side_effects=True, vmem_limit_bytes=62 * 2**20),
        name="backward",
    )(*args)
    return outs

def solution(mesh):
    def step(x, dy, *arrays):
        weights, m, v = (arrays[i : i + 7] for i in (0, 7, 14))
        a, q, k, val, o, lse, hm, b, h1 = forward(x[0], *weights)
        return tuple(backward("dp", dy[0], (b, hm, a, q, k, val, o, lse), h1, weights, m, v))

    states, all_of, cut = P(("rep", "dp"), None, None), P(None, None, None), P(None, "dp", None)
    return jax.shard_map(
        step,
        mesh=mesh,
        in_specs=(states, states) + (all_of,) * 7 + (cut,) * 14,
        out_specs=(P("rep", None, None),) * 7 + (P("rep", "dp", None),) * 14,
        check_vma=False,
    )
```

```python
import functools

import jax
import jax.numpy as jnp
import numpy as np
from jax import lax
from jax.experimental import pallas as pl
from jax.experimental.pallas import tpu as pltpu
from jax.sharding import PartitionSpec as P

F32, BF16 = jnp.float32, jnp.bfloat16


HEAD = 128
THETA = 10000
LOG2E = 1.4426950408889634
NEG = -1e30
HIDDEN = 2 * NEG
TB = 512


def dot(a, b, ca=1, cb=0):
    return lax.dot_general(a, b, (((ca,), (cb,)), ((), ())), preferred_element_type=F32)


def rotary_tables(tokens):
    half = HEAD // 2
    rate = float(THETA) ** (-np.arange(half) / half)
    rate = np.concatenate([rate, rate])
    turn = np.concatenate([-np.ones(half), np.ones(half)])
    big = np.arange(tokens // 64)[:, None] * 64.0 * rate
    small = np.arange(64)[:, None] * rate
    return [jnp.asarray(t, F32) for t in (np.cos(big), np.sin(big), np.cos(small), np.sin(small))], jnp.asarray(turn[None], F32)


def fill_rotary(tabs, at, cos_s, sin_s):
    cb_ref, sb_ref, cs_ref, ss_ref, turn_ref = tabs
    cs, ss, turn = cs_ref[...], ss_ref[...], turn_ref[...]
    for n in range(TB // 64):
        cb, sb = cb_ref[pl.ds(at * (TB // 64) + n, 1), :], sb_ref[pl.ds(at * (TB // 64) + n, 1), :]
        cos_s[n * 64 : n * 64 + 64, :] = cb * cs - sb * ss
        sin_s[n * 64 : n * 64 + 64, :] = (sb * cs + cb * ss) * turn


def rotated(t, cos, sin):
    return t * cos + pltpu.roll(t, HEAD // 2, 1) * sin


def normed(h):
    wide = h.astype(F32)
    scale = lax.rsqrt(jnp.mean(wide * wide, -1, keepdims=True) + 1e-6)
    return (wide * scale).astype(BF16)


def attend_block(nb, q_s, k_ref, v_ref, o_put, lse_put, top_s, mix_s):
    heads = q_s.shape[1] // HEAD
    e = HEAD**-0.5 * LOG2E
    ones = jnp.ones((8, TB), BF16)

    def block(j):
        here = pl.ds(pl.multiple_of(j * TB, TB), TB)
        scores = [dot(k_ref[here, h * HEAD : h * HEAD + HEAD], q_s[:, h * HEAD : h * HEAD + HEAD], 1, 1) for h in range(heads)]
        weights, keeps = [], []
        for h, s in enumerate(scores):
            old = top_s[h : h + 1, :]
            top = jnp.maximum(old, s.max(axis=0, keepdims=True))
            keeps.append(jnp.exp2((old - top) * e))
            top_s[h : h + 1, :] = top
            weights.append(jnp.exp2((s - top) * e).astype(BF16))
        for h, p in enumerate(weights):
            values = jnp.concatenate([v_ref[here, h * HEAD : h * HEAD + HEAD].T, ones], axis=0)
            mix_s[h] = mix_s[h] * keeps[h] + dot(values, p)

    def diagonal():
        half = TB // 2
        early = pl.ds(pl.multiple_of(nb * TB, TB), half)
        late = pl.ds(pl.multiple_of(nb * TB + half, half), half)
        cols = [slice(h * HEAD, h * HEAD + HEAD) for h in range(heads)]
        ok = lax.broadcasted_iota(jnp.int32, (half, TB), 1) >= lax.broadcasted_iota(jnp.int32, (half, TB), 0)
        seen = [jnp.where(ok, dot(k_ref[early, c], q_s[:, c], 1, 1), HIDDEN) for c in cols]
        more = [jnp.where(ok[:, :half], dot(k_ref[late, c], q_s[half:, c], 1, 1), HIDDEN) for c in cols]
        weights = []
        for h, (s, t) in enumerate(zip(seen, more)):
            top = s.max(axis=0, keepdims=True)
            top = jnp.concatenate([top[:, :half], jnp.maximum(top[:, half:], t.max(axis=0, keepdims=True))], axis=1)
            top_s[h : h + 1, :] = top
            weights.append((jnp.exp2((s - top) * e).astype(BF16), jnp.exp2((t - top[:, half:]) * e).astype(BF16)))
        for h, (c, (p, r)) in enumerate(zip(cols, weights)):
            got = dot(jnp.concatenate([v_ref[early, c].T, ones[:, :half]], axis=0), p)
            mix_s[h, :, :half] = got[:, :half]
            mix_s[h, :, half:] = got[:, half:] + dot(jnp.concatenate([v_ref[late, c].T, ones[:, :half]], axis=0), r)

    diagonal()
    lax.fori_loop(0, nb, lambda j, _: block(j), None)
    for h in range(heads):
        total = mix_s[h, HEAD : HEAD + 1, :]
        o_put(h, (mix_s[h, :HEAD, :] * (1 / total)).T.astype(BF16))
        lse_put(h, top_s[h : h + 1, :] * (HEAD**-0.5) + jnp.log(total))


def forward_kernel(x_ref, *refs, ff):
    w_h, tabs, refs = refs[:7], refs[7:12], refs[12:]
    out_h, refs = refs[:9], refs[9:]
    w_s, (stage, lse_s, ks, vs, cos_s, sin_s, top_s, mix_s, w_sem, out_sem) = refs[:7], refs[7:]
    wq_s, wk_s, wv_s, wo_s, wg_s, wu_s, wd_s = w_s
    i, last = pl.program_id(0), pl.num_programs(0) - 1
    d = x_ref.shape[1]
    heads = d // HEAD
    at = lax.rem(i, 2)
    here = pl.ds(pl.multiple_of(i * TB, TB), TB)
    fill_rotary(tabs, i, cos_s, sin_s)

    loads = [pltpu.make_async_copy(w_h[n].at[0] if n > 3 else w_h[n], w_s[n], w_sem.at[n]) for n in (0, 1, 2, 3, 4, 5, 6)]

    def saves(slot, block):
        rows = pl.ds(pl.multiple_of(block * TB, TB), TB)
        whole = [pltpu.make_async_copy(stage.at[slot, n, layer], out_h[n].at[layer, rows, :], out_sem.at[slot, n, layer]) for n in range(7) for layer in range(2)]
        lse = [pltpu.make_async_copy(lse_s.at[slot, layer], out_h[7].at[layer, :, rows], out_sem.at[slot, 7, layer]) for layer in range(2)]
        return whole + lse + [pltpu.make_async_copy(stage.at[slot, 7, 0], out_h[8].at[rows, :], out_sem.at[slot, 8, 0])]

    def put(n, layer, value):
        stage[at, n, layer] = value
        saves(at, i)[2 * n + layer].start()

    @pl.when(i == 0)
    def _():
        for copy in loads:
            copy.start()
        for copy in loads[:3]:
            copy.wait()

    @pl.when(i >= 2)
    def _():
        for copy in saves(at, i - 2):
            copy.wait()

    def attention_part(layer, h):
        a = normed(h)
        put(0, layer, a)
        for n, (w, kept) in enumerate(((wq_s, None), (wk_s, ks), (wv_s, vs))):
            t = dot(a, w[layer]).astype(BF16)
            if n < 2:
                cos, sin = cos_s[...], sin_s[...]
                wide = t.astype(F32)
                t = jnp.concatenate([rotated(wide[:, m * HEAD : m * HEAD + HEAD], cos, sin) for m in range(heads)], axis=1).astype(BF16)
            put(1 + n, layer, t)
            if kept is not None:
                kept[layer, here, :] = t

        def o_put(m, o):
            stage[at, 4, layer, :, m * HEAD : m * HEAD + HEAD] = o

        def lse_put(m, lse):
            lse_s[at, layer, m : m + 1, :] = lse

        attend_block(i, stage.at[at, 1, layer], ks.at[layer], vs.at[layer], o_put, lse_put, top_s, mix_s)
        saves(at, i)[2 * 4 + layer].start()
        saves(at, i)[2 * 7 + layer].start()
        if layer == 0:
            @pl.when(i == 0)
            def _():
                for copy in loads[3:]:
                    copy.wait()
        hm = h + dot(stage[at, 4, layer], wo_s[layer]).astype(BF16)
        put(5, layer, hm)
        b = normed(hm)
        put(6, layer, b)
        return hm, b

    hm, b = attention_part(0, x_ref[...])
    total = None
    step = 512
    for n in range(0, ff, step):
        gate, up = dot(b, wg_s[:, n : n + step]), dot(b, wu_s[:, n : n + step])
        part = dot((gate * jax.nn.sigmoid(gate) * up).astype(BF16), wd_s[n : n + step, :])
        total = part if total is None else total + part
    h1 = hm + total.astype(BF16)
    stage[at, 7, 0] = h1
    saves(at, i)[16].start()
    attention_part(1, h1)

    @pl.when(i == last)
    def _():
        for copy in saves(1 - at, i - 1) + saves(at, i):
            copy.wait()


def forward(x, *weights):
    tokens, d = x.shape
    ff = weights[4].shape[2]
    heads = d // HEAD
    tabs, turn = rotary_tables(tokens)
    whole = lambda a: pl.BlockSpec(a.shape, lambda i: (0,) * a.ndim, pipeline_mode=pl.Buffered(1))
    anywhere = pl.BlockSpec(memory_space=pltpu.HBM)
    big = jax.ShapeDtypeStruct((2, tokens, d), BF16)
    sem = pltpu.SemaphoreType.DMA
    vmem = pltpu.VMEM
    return pl.pallas_call(
        functools.partial(forward_kernel, ff=ff),
        grid=(tokens // TB,),
        in_specs=[pl.BlockSpec((TB, d), lambda i: (i, 0)), *[anywhere] * 7, *(whole(t) for t in (*tabs, turn))],
        out_specs=[anywhere] * 9,
        out_shape=[big] * 7 + [jax.ShapeDtypeStruct((2, heads, tokens), F32), jax.ShapeDtypeStruct((tokens, d), BF16)],
        scratch_shapes=[*(vmem(w.shape[n > 3 :], BF16) for n, w in enumerate(weights)), vmem((2, 8, 2, TB, d), BF16), vmem((2, 2, heads, TB), F32),
                        vmem((2, tokens, d), BF16), vmem((2, tokens, d), BF16), vmem((TB, HEAD), F32), vmem((TB, HEAD), F32),
                        vmem((heads, TB), F32), vmem((heads, HEAD + 8, TB), F32), sem((7,)), sem((2, 9, 2))],
        compiler_params=pltpu.CompilerParams(dimension_semantics=("arbitrary",), vmem_limit_bytes=60 * 2**20),
        name="forward",
    )(x, *(pltpu.with_memory_space_constraint(w, pltpu.HBM) for w in weights), *tabs, turn)

N = 8
ROWS, COLS = 64, 512
SLOTS = 8
MESH = pl.DeviceIdType.MESH


class Ring:
    def __init__(self, axis, count, terms, rs, new, sems, term_at, update):
        self.axis, self.count = axis, count
        self.terms, self.rs, self.new, self.sems = terms, rs, new, sems
        self.term_at, self.update = term_at, update
        self.me = lax.axis_index(axis)

    def at(self, offset):
        return lax.rem(self.me + offset + 2 * N, N)

    def barrier(self):
        sem = pltpu.get_barrier_semaphore()
        for d in (1, -1):
            pl.semaphore_signal(sem, inc=1, device_id={self.axis: self.at(d)}, device_id_type=MESH)
        pl.semaphore_wait(sem, 2)

    def sign(self, c):
        return 1 - 2 * lax.rem(c, 2)

    def copy(self, which, c, s, far):
        at, slot = lax.rem(c, SLOTS), (0 if far else 4) + s - 1
        d = self.sign(c) * (1 if far else -1)
        if which == 0:
            block = self.at(d * ((4 if far else 3) - s + 1))
            src = self.terms.at[self.term_at(c), block] if s == 1 else self.rs.at[at, slot - 1]
            dst = self.rs.at[at, slot]
        else:
            d = -d
            src = dst = self.new.at[c, self.at(-d * (s - 1))]
        return pltpu.make_async_remote_copy(src_ref=src, dst_ref=dst, send_sem=self.sems[2 * which].at[at, slot], recv_sem=self.sems[2 * which + 1].at[at, slot],
                                            device_id={self.axis: self.at(d)}, device_id_type=MESH)

    def step(self, which, c, age):
        at = lax.rem(c, SLOTS)
        for far in (True, False):
            hops = 4 if far else 3
            if age > hops:
                continue
            if age > 0:
                self.copy(which, c, age, far).wait()
            if which == 0 and 0 < age < hops:
                block = self.at(self.sign(c) * (1 if far else -1) * (hops - age))
                got = self.rs.at[at, (0 if far else 4) + age - 1]
                got[...] = (got[...].astype(F32) + self.terms[self.term_at(c), block].astype(F32)).astype(BF16)
            if age < hops:
                self.copy(which, c, age + 1, far).start()
        if which == 0 and age == 4:
            g = self.terms[self.term_at(c), self.me].astype(F32) + self.rs[at, 3].astype(F32) + self.rs[at, 6].astype(F32)
            self.new[c, self.me] = self.update(c, g.astype(BF16))

    def each(self, c, does):
        @pl.when((c >= 0) & (c < self.count))
        def _(): does(c)

    def tick(self, t):
        for which, ages in ((0, range(5)), (1, range(5))):
            for age in ages:
                self.each(t - 4 * which - age, lambda c, which=which, age=age: self.step(which, c, age))

FB = 256
PER = 16
KEEP = 4


def adamw(w, m, v, g):
    m = 0.9 * m + 0.1 * g
    v = 0.95 * v + 0.05 * g * g
    return (w - 0.02 * (m * lax.rsqrt(v + 1e-8) + 0.1 * w)).astype(BF16), m, v


def term_slot(k):
    if isinstance(k, int):
        return k if k < PER - 4 else k - 9
    return jnp.where(k < PER - 4, k, k - 9)


def norm_back(by_n, h):
    scale = lax.rsqrt(jnp.mean(h * h, -1, keepdims=True) + 1e-6)
    return by_n * scale - h * (scale * scale * scale * jnp.mean(by_n * h, -1, keepdims=True))


def backward_kernel(*refs, axis, tokens, d, ff, layers):
    (dy_h, b_h, hm_h, a_h, q_h, k_h, v_h, o_h, lse_h, h1_h), refs = refs[:10], refs[10:]
    weights_h, m_h, v2_h, tabs, refs = refs[:7], refs[7:14], refs[14:21], refs[21:26], refs[26:]
    (new, F1, F2), refs = refs[:3], refs[3:]
    (S1, S2, S3, S4, S5, S6, g_s, dq_s, lse_s, delta_s, wa_s, wgu_s, wd_s, cos_s, sin_s,
     terms, rs, mw_s, w_s, rs_send, rs_recv, ag_send, ag_recv, in_sem, act_sem, slab_sem, mom_sem) = refs
    wq_h, wk_h, wv_h, wo_h, wg_h, wu_h, wd_h = weights_h
    heads = d // HEAD
    steps, blocks = ff // FB, tokens // TB
    count = layers * PER
    me = lax.axis_index(axis)

    def kinds(c):
        k = lax.rem(c, PER)
        layer = layers - 1 - lax.div(c, PER)
        return k, layer

    def places(c, owner, arrays, mine):
        k, layer = kinds(c)
        q, kk, v, o, g, u, dn = arrays
        own = 0 if mine else owner
        slab = pl.ds(pl.multiple_of(jnp.minimum(k, steps - 1) * FB, FB), FB)
        rows = pl.ds(pl.multiple_of(own * ROWS, ROWS), ROWS)
        strip = pl.ds(pl.multiple_of(own * (ff // N) + jnp.clip(k - steps, 0, 3) * ROWS, ROWS), ROWS)
        out = [(k < steps, [(g.at[layer, rows, slab], 0, FB), (u.at[layer, rows, slab], FB, FB)]),
               ((k >= steps) & (k < steps + 4), [(dn.at[layer, strip, :], 0, COLS)])]
        for n, ref in enumerate((o, q, kk, v)):
            out.append((k == steps + 4 + n, [(ref.at[layer, rows, :], 0, COLS)]))
        return out

    def pull(c, arrays, mine, dst, sem):
        for cond, parts in places(c, me, arrays, mine):
            @pl.when(cond)
            def _():
                for ref, col, cols in parts:
                    pltpu.make_async_copy(ref, dst.at[:, pl.ds(col, cols)], sem).start()

    def pulled(dst, sem):
        pltpu.make_async_copy(dst, dst, sem).wait()

    def fetch(c):
        at = lax.rem(c, KEEP)
        for n, arrays in enumerate((m_h, v2_h)):
            pull(c, arrays, True, mw_s.at[at, n], in_sem.at[at, n])
        pull(c, weights_h, False, w_s.at[at], in_sem.at[at, 2])

    def update(c, g):
        at = lax.rem(c, KEEP)
        for n, dst in enumerate((mw_s.at[at, 0], mw_s.at[at, 1], w_s.at[at])):
            pulled(dst, in_sem.at[at, n])
        g_s[c] = g
        return adamw(w_s[at].astype(F32), mw_s[at, 0], mw_s[at, 1], g.astype(F32))[0]

    ring = Ring(axis, count, terms, rs, new, (rs_send, rs_recv, ag_send, ag_recv), lambda c: term_slot(lax.rem(c, PER)), update)

    def tick(t):
        ring.each(t - 2, fetch)
        ring.tick(t)

    def slab(layer, j, at):
        here = pl.ds(pl.multiple_of(j * FB, FB), FB)
        return [pltpu.make_async_copy(wg_h.at[layer, :, here], wgu_s.at[at, :, 0:FB], slab_sem.at[at, 0]),
                pltpu.make_async_copy(wu_h.at[layer, :, here], wgu_s.at[at, :, FB : 2 * FB], slab_sem.at[at, 1]),
                pltpu.make_async_copy(wd_h.at[layer, here, :], wd_s.at[at], slab_sem.at[at, 2])]

    def load(n, ref, dst):
        return pltpu.make_async_copy(ref, dst, act_sem.at[n])

    def attention_weights(layer):
        return [load(8 + n, w.at[layer], wa_s.at[n]) for n, w in enumerate((wq_h, wk_h, wv_h, wo_h))]

    top = layers - 1
    load(0, b_h.at[top], S1).start()
    load(1, dy_h, S2).start()
    for copy in slab(top, 0, 0):
        copy.start()
    ring.barrier()
    load(1, dy_h, S2).wait()

    def mlp_step(p, layer, j):
        at = lax.rem(j, 2)
        for copy in slab(layer, j, at):
            copy.wait()
        @pl.when(j + 1 < steps)
        def _():
            for copy in slab(layer, j + 1, 1 - at):
                copy.start()

        rows = [pl.ds(i * TB, TB) for i in range(blocks)]

        def first(i):
            return dot(S1[rows[i], :], wgu_s[at]), dot(S2[rows[i], :], wd_s[at], 1, 1)

        def second(i, gu, by_act):
            by_act = by_act.astype(BF16).astype(F32)
            gate, up = gu[:, :FB], gu[:, FB:]
            s = jax.nn.sigmoid(gate)
            gs = gate * s
            S4[rows[i], 0:FB] = (gs * up).astype(BF16)
            S3[rows[i], :] = jnp.concatenate([by_act * up * (s + gs * (1 - s)), by_act * gs], axis=1).astype(BF16)

        def third(i):
            F1[rows[i], :] = jnp.where(j > 0, F1[rows[i], :], 0.0) + dot(S3[rows[i], :], wgu_s[at], 1, 1)

        ahead = first(0)
        for i in range(blocks):
            now, ahead = ahead, first(i + 1) if i + 1 < blocks else None
            second(i, *now)

        put_terms(j, dot(S1[...], S3[...], 0, 0).astype(BF16))
        tick(p * PER + j)
        by_d = dot(S4[:, 0:FB], S2[...], 0, 0).astype(BF16)
        for r in range(FB // ROWS):
            terms[steps + r, j] = by_d[r * ROWS : (r + 1) * ROWS, :]
        for i in range(blocks):
            third(i)

    def put_terms(k, by_w):
        for r in range(N):
            terms[term_slot(k), r] = by_w[r * ROWS : (r + 1) * ROWS, :]

    def turned_back(t, cos, sin):
        parts = [rotated(t[:, n * HEAD : n * HEAD + HEAD], cos, -sin) for n in range(heads)]
        return jnp.concatenate(parts, axis=1).astype(BF16)

    def one_layer(p, _):
        layer = layers - 1 - p
        for copy in attention_weights(layer):
            copy.start()
        load(2, hm_h.at[layer], S6).start()
        load(3, o_h.at[layer], S5).start()
        load(5, lse_h.at[layer], lse_s).start()
        load(0, b_h.at[layer], S1).wait()
        lax.fori_loop(0, steps, lambda j, _: mlp_step(p, layer, j), None)
        load(0, q_h.at[layer], S1).start()
        load(6, k_h.at[layer], S3).start()
        load(7, v_h.at[layer], S4).start()
        for copy in attention_weights(layer):
            copy.wait()
        load(2, hm_h.at[layer], S6).wait()
        load(3, o_h.at[layer], S5).wait()
        load(5, lse_h.at[layer], lse_s).wait()

        def into_attention(i, _):
            here = pl.ds(pl.multiple_of(i * TB, TB), TB)
            by_b = F1[here, :].astype(BF16).astype(F32)
            back = norm_back(by_b, S6[here, :].astype(F32)).astype(BF16)
            by_hm = (S2[here, :].astype(F32) + back.astype(F32)).astype(BF16)
            S2[here, :] = by_hm
            by_o = dot(by_hm, wa_s[3], 1, 1).astype(BF16)
            S6[here, :] = by_o
            both = (by_o.astype(F32) * S5[here, :].astype(F32)).T
            for h in range(heads):
                delta_s[h : h + 1, here] = both[h * HEAD : h * HEAD + HEAD, :].sum(axis=0, keepdims=True)

        lax.fori_loop(0, blocks, into_attention, None)
        put_terms(steps + 4, dot(S5[...], S2[...], 0, 0).astype(BF16))
        load(0, q_h.at[layer], S1).wait()
        load(6, k_h.at[layer], S3).wait()
        load(7, v_h.at[layer], S4).wait()

        e = HEAD**-0.5 * LOG2E

        def pair(i, j, masked):
            qs = pl.ds(pl.multiple_of(i * TB, TB), TB)
            ks = pl.ds(pl.multiple_of(j * TB, TB), TB)
            cols = [slice(h * HEAD, h * HEAD + HEAD) for h in range(heads)]
            scores = [dot(S3[ks, c], S1[qs, c], 1, 1) for c in cols]
            dps = [dot(S4[ks, c], S6[qs, c], 1, 1) for c in cols]
            if masked:
                ok = lax.broadcasted_iota(jnp.int32, (TB, TB), 1) >= lax.broadcasted_iota(jnp.int32, (TB, TB), 0)
            for h, c in enumerate(cols):
                prob = jnp.exp2(scores[h] * e - lse_s[h : h + 1, qs] * LOG2E)
                if masked:
                    prob = jnp.where(ok, prob, 0.0)
                ds = (prob * (dps[h] - delta_s[h : h + 1, qs])).astype(BF16)
                by_v = dot(prob.astype(BF16), S6[qs, c])
                by_k = dot(ds, S1[qs, c])
                if masked:
                    F2[ks, c] = by_v
                    F1[ks, c] = by_k
                else:
                    F2[ks, c] += by_v
                    F1[ks, c] += by_k
                dq_s[h] += dot(S3[ks, c].T, ds)

        def flat(n, _):
            i = (n >= 1).astype(jnp.int32) + (n >= 3).astype(jnp.int32) + (n >= 6).astype(jnp.int32)
            j = n - lax.div(i * (i + 1), 2)
            @pl.when(j == 0)
            def _(): dq_s[...] = jnp.zeros_like(dq_s)
            @pl.when(j < i)
            def _(): pair(i, j, False)
            @pl.when(j == i)
            def _():
                pair(i, j, True)
                qs = pl.ds(pl.multiple_of(i * TB, TB), TB)
                fill_rotary(tabs, i, cos_s, sin_s)
                by_q = jnp.concatenate([(dq_s[h] * HEAD**-0.5).T for h in range(heads)], axis=1).astype(BF16).astype(F32)
                S5[qs, :] = turned_back(by_q, cos_s[...], sin_s[...])
            @pl.when(lax.rem(n, 2) == 0)
            def _(): tick(p * PER + steps + lax.div(n, 2))

        lax.fori_loop(0, blocks * (blocks + 1) // 2, flat, None)

        load(4, a_h.at[layer], S6).start()

        @pl.when(p + 1 < layers)
        def _():
            load(0, b_h.at[layer - 1], S1).start()
            for copy in slab(layer - 1, 0, 0):
                copy.start()

        def out_of_attention(i, _):
            here = pl.ds(pl.multiple_of(i * TB, TB), TB)
            fill_rotary(tabs, i, cos_s, sin_s)
            S3[here, :] = turned_back((F1[here, :] * HEAD**-0.5).astype(BF16).astype(F32), cos_s[...], sin_s[...])
            S4[here, :] = F2[here, :].astype(BF16)

        lax.fori_loop(0, blocks, out_of_attention, None)
        load(4, a_h.at[layer], S6).wait()
        for n, ref in enumerate((S5, S3, S4)):
            put_terms(steps + 5 + n, dot(S6[...], ref[...], 0, 0).astype(BF16))
            if n == 2:
                load(2, h1_h, S6).start()
            tick(p * PER + steps + 5 + n)

        load(2, h1_h, S6).wait()

        @pl.when(p + 1 < layers)
        def _():

            def into_layer(i, _):
                here = pl.ds(pl.multiple_of(i * TB, TB), TB)
                by_a = sum(dot(ref[here, :], wa_s[n], 1, 1) for n, ref in enumerate((S5, S3, S4))).astype(BF16).astype(F32)
                back = norm_back(by_a, S6[here, :].astype(F32)).astype(BF16)
                S2[here, :] = (S2[here, :].astype(F32) + back.astype(F32)).astype(BF16)

            lax.fori_loop(0, blocks, into_layer, None)

    lax.fori_loop(0, layers, one_layer, None)
    def moments(c):
        return pl.ds(pl.multiple_of(c * ROWS, ROWS), ROWS)

    def fetch_moments(c, _):
        for n, (arrays, out) in enumerate(((m_h, F1), (v2_h, F2))):
            pull(c, arrays, True, out.at[moments(c), :], mom_sem.at[n])

    lax.fori_loop(0, count, fetch_moments, None)
    tick(count)
    for n, out in enumerate((F1, F2)):
        pulled(out, mom_sem.at[n])

    def last(t, _):
        tick(t)
        for n in range(KEEP):
            c = (t - count - 1) * KEEP + n
            here = moments(c)
            _, m, v = adamw(0.0, F1[here, :], F2[here, :], g_s[c].astype(F32))
            F1[here, :] = m
            F2[here, :] = v

    lax.fori_loop(count + 1, count + 1 + count // KEEP, last, None)


def backward(axis, dy, kept, h1, weights, m, v):
    layers, tokens, d = kept[0].shape
    ff = weights[4].shape[2]
    tabs, turn = rotary_tables(tokens)
    args = [dy, *kept, h1, *weights, *m, *v, *tabs, turn]
    anywhere = pl.BlockSpec(memory_space=pltpu.HBM)
    inside = pl.BlockSpec(memory_space=pltpu.VMEM)
    big = lambda t: pltpu.VMEM((tokens, d), t)
    sem = pltpu.SemaphoreType.DMA
    return pl.pallas_call(
        functools.partial(backward_kernel, axis=axis, tokens=tokens, d=d, ff=ff, layers=layers),
        in_specs=[anywhere] * (len(args) - 5) + [inside] * 5,
        out_shape=[pltpu.VMEM((layers * PER, N, ROWS, COLS), BF16), big(F32), big(F32)],
        scratch_shapes=[*(big(BF16) for _ in range(6)), pltpu.VMEM((layers * PER, ROWS, COLS), BF16), pltpu.VMEM((d // HEAD, HEAD, TB), F32),
                        pltpu.VMEM((d // HEAD, tokens), F32), pltpu.VMEM((d // HEAD, tokens), F32), pltpu.VMEM((4, d, d), BF16),
                        pltpu.VMEM((2, d, 2 * FB), BF16), pltpu.VMEM((2, FB, d), BF16), pltpu.VMEM((TB, HEAD), F32), pltpu.VMEM((TB, HEAD), F32),
                        pltpu.VMEM((PER - 4, N, ROWS, COLS), BF16), pltpu.VMEM((SLOTS, 7, ROWS, COLS), BF16),
                        pltpu.VMEM((KEEP, 2, ROWS, COLS), F32), pltpu.VMEM((KEEP, ROWS, COLS), BF16),
                        sem((SLOTS, 7)), sem((SLOTS, 7)), sem((SLOTS, 7)), sem((SLOTS, 7)), sem((KEEP, 3)), sem((12,)), sem((2, 3)), sem((2,))],
        compiler_params=pltpu.CompilerParams(collective_id=0, has_side_effects=True, vmem_limit_bytes=39 * 2**20),
        name="backward",
    )(*args)


def finish_kernel(new, m_ref, v_ref, *refs, layers, ff):
    new_h, nm_h, nv_h, (sem, m_sem, v_sem) = refs[:7], refs[7:14], refs[14:21], refs[21:]
    steps = ff // FB
    copies = []

    def put(c, n, cols, at):
        own = pl.ds(c * ROWS, ROWS)
        mine, whole = at[:1] + at[2:], at
        copies.append(pltpu.make_async_copy(new.at[c, :, :, cols], new_h[n].at[whole], sem))
        copies.append(pltpu.make_async_copy(m_ref.at[own, cols], nm_h[n].at[mine], m_sem))
        copies.append(pltpu.make_async_copy(v_ref.at[own, cols], nv_h[n].at[mine], v_sem))

    every = slice(None)
    for p in range(layers):
        layer, base = layers - 1 - p, p * PER
        for k in range(steps):
            for n in range(2):
                put(base + k, 4 + n, pl.ds(n * FB, FB), (layer, every, every, pl.ds(k * FB, FB)))
        for r in range(4):
            put(base + steps + r, 6, every, (layer, every, r))
            put(base + steps + 4 + r, (3, 0, 1, 2)[r], every, (layer,))
    for copy in copies:
        copy.start()
    for ref, one in ((new, sem), (m_ref, m_sem), (v_ref, v_sem)):
        pltpu.make_async_copy(ref, ref, one).wait()


def finish(new, moment, square, weights, m, v):
    layers, d, ff = weights[4].shape
    inside = pl.BlockSpec(memory_space=pltpu.VMEM)
    sem = pltpu.SemaphoreType.DMA
    shape = lambda s, t: jax.ShapeDtypeStruct(s, t)
    rows = [(ROWS, d)] * 4 + [(ROWS, ff)] * 2 + [(4, ROWS, d)]
    outs = pl.pallas_call(
        functools.partial(finish_kernel, layers=layers, ff=ff),
        in_specs=[inside] * 3,
        out_specs=[pl.BlockSpec(memory_space=pltpu.HBM)] * 21,
        out_shape=[shape((layers, N, *s), BF16) for s in rows] + [shape((layers, *s), F32) for s in rows] * 2,
        scratch_shapes=[sem, sem, sem],
        compiler_params=pltpu.CompilerParams(vmem_limit_bytes=2**20),
        name="finish",
    )(new, moment, square)
    return [one.reshape(a.shape) for one, a in zip(outs, (*weights, *m, *v))]

def solution(mesh):
    def step(x, dy, *arrays):
        weights, m, v = (arrays[i : i + 7] for i in (0, 7, 14))
        a, q, k, val, o, hm, b, lse, h1 = forward(x[0], *weights)
        return tuple(finish(*backward("dp", dy[0], (b, hm, a, q, k, val, o, lse), h1, weights, m, v), weights, m, v))

    states, all_of, cut = P(("rep", "dp")), P(), P(None, "dp")
    return jax.shard_map(
        step,
        mesh=mesh,
        in_specs=(states, states) + (all_of,) * 7 + (cut,) * 14,
        out_specs=(P("rep"),) * 7 + (P("rep", "dp"),) * 14,
        check_vma=False,
    )
```
